64 devices in a mesh: rep: 4 (over x, y), dp: 16 (over z, core).
Axes of the slice: x: 2, y: 2, z: 8, core: 2. Of those that a mesh axis runs over, the one named last changes fastest.
The devices are a block of a 4x4x8 slice.
Arguments:
- g_w_gate: bfloat16 [64, 2, 512, 8192], P(('rep', 'dp')), parts along dimension 0
- g_w_up: bfloat16 [64, 2, 512, 8192], P(('rep', 'dp')), parts along dimension 0
- g_w_down: bfloat16 [64, 2, 8192, 512], P(('rep', 'dp')), parts along dimension 0
- w_gate: bfloat16 [2, 512, 8192], replicated
- w_up: bfloat16 [2, 512, 8192], replicated
- w_down: bfloat16 [2, 8192, 512], replicated
- m_w_gate: float32 [2, 512, 8192], P(None, 'dp')
- m_w_up: float32 [2, 512, 8192], P(None, 'dp')
- m_w_down: float32 [2, 8192, 512], P(None, 'dp')
- v_w_gate: float32 [2, 512, 8192], P(None, 'dp')
- v_w_up: float32 [2, 512, 8192], P(None, 'dp')
- v_w_down: float32 [2, 8192, 512], P(None, 'dp')
Outputs:
- output 1: bfloat16 [8, 512, 8192], P('rep'), parts along dimension 0
- output 2: bfloat16 [8, 512, 8192], P('rep'), parts along dimension 0
- output 3: bfloat16 [8, 8192, 512], P('rep'), parts along dimension 0
- output 4: float32 [8, 512, 8192], P('rep', 'dp'), parts along dimension 0
- output 5: float32 [8, 512, 8192], P('rep', 'dp'), parts along dimension 0
- output 6: float32 [8, 8192, 512], P('rep', 'dp'), parts along dimension 0
- output 7: float32 [8, 512, 8192], P('rep', 'dp'), parts along dimension 0
- output 8: float32 [8, 512, 8192], P('rep', 'dp'), parts along dimension 0
- output 9: float32 [8, 8192, 512], P('rep', 'dp'), parts along dimension 0
There are 4 independent parts. The reference program is written for one: setup_inputs(seed, part) draws one part's arguments, and reference() takes and returns one part's arrays. A program takes and returns all parts, laid end to end along the dimension named above; an argument that names none is the same for every part.
All inputs are finite; a program needn't handle non-finite values.
Results may differ from the reference program's by a relative error of at most 0.022.
Values are sent between devices in bfloat16 or wider.
A program may use at most 768 MiB of HBM per device.

```python
import jax
import jax.numpy as jnp
from jax import lax

DEVICES = 16
D = 512
FF = 8192
LAYERS = 2
NAMES = ("w_gate", "w_up", "w_down")
SHAPES = {"w_gate": (LAYERS, D, FF), "w_up": (LAYERS, D, FF), "w_down": (LAYERS, FF, D)}


def setup_inputs(seed: int = 0, part: int = 0) -> dict:
    kz, *keys = jax.random.split(jax.random.key(seed), 1 + 5 * len(NAMES))
    loud = 2.0 ** jax.random.uniform(kz, (), jnp.float32, -1.0, 1.0)
    drawn = {}
    for name, key, both in zip(NAMES, keys[:3], keys[3:6], strict=True):
        own = jax.random.normal(jax.random.fold_in(key, part), (DEVICES, *SHAPES[name]), jnp.float32)
        shared = jax.random.normal(jax.random.fold_in(both, part), SHAPES[name], jnp.float32)
        drawn["g_" + name] = (loud * (0.7 * shared / DEVICES + 0.7 * own * DEVICES**-0.5)).astype(jnp.bfloat16)
    for name, key in zip(NAMES, keys[6:9], strict=True):
        drawn[name] = (jax.random.normal(key, SHAPES[name], jnp.float32) * SHAPES[name][1] ** -0.5).astype(jnp.bfloat16)
    for name, key in zip(NAMES, keys[9:12], strict=True):
        drawn["m_" + name] = loud * 0.5 * jax.random.normal(key, SHAPES[name], jnp.float32)
    for name, key in zip(NAMES, keys[12:15], strict=True):
        drawn["v_" + name] = loud * loud * jax.random.uniform(key, SHAPES[name], jnp.float32, 0.5, 1.5)
    return drawn


def adamw(w, m, v, g):
    m = 0.9 * m + 0.1 * g
    v = 0.95 * v + 0.05 * g * g
    step = m * lax.rsqrt(v + 1e-8) + 0.1 * w
    return (w - 0.02 * step).astype(jnp.bfloat16), m, v


def reference(g_w_gate, g_w_up, g_w_down, w_gate, w_up, w_down, m_w_gate, m_w_up, m_w_down, v_w_gate, v_w_up, v_w_down):
    def total(terms):
        return lax.scan(lambda so_far, term: (so_far + term.astype(jnp.float32), None), jnp.zeros(terms.shape[1:], jnp.float32), terms)[0]

    gradients = [total(terms).astype(jnp.bfloat16).astype(jnp.float32) for terms in (g_w_gate, g_w_up, g_w_down)]
    new = [
        adamw(w.astype(jnp.float32), m, v, g)
        for w, m, v, g in zip((w_gate, w_up, w_down), (m_w_gate, m_w_up, m_w_down), (v_w_gate, v_w_up, v_w_down), gradients, strict=True)
    ]
    return tuple(one[which] for which in range(3) for one in new)
```

```python
import functools

import jax
import jax.numpy as jnp
from jax import lax
from jax.experimental import pallas as pl
from jax.experimental.pallas import tpu as pltpu
from jax.sharding import PartitionSpec as P

CORES = 2
LAYERS = 2
NAMES = 3
CHUNK = 32768
MESH = pl.DeviceIdType.MESH


def adamw(w, m, v, g):
    m = 0.9 * m + 0.1 * g
    v = 0.95 * v + 0.05 * g * g
    step = m * lax.rsqrt(v + 1e-8) + 0.1 * w
    return (w - 0.02 * step).astype(jnp.bfloat16), m, v


def chunks(shape, body):
    rows, columns = shape
    if columns * rows <= CHUNK:
        body((slice(None), slice(None)))
    elif rows * 128 <= CHUNK and columns % (CHUNK // rows) == 0:
        size = CHUNK // rows

        @pl.loop(0, columns // size)
        def _(i):
            body((slice(None), pl.ds(pl.multiple_of(i * size, size), size)))
    else:
        size = CHUNK // columns

        @pl.loop(0, rows // size)
        def _(i):
            body((pl.ds(pl.multiple_of(i * size, size), size), slice(None)))


def kernel(n, *refs):
    groups = [refs[i : i + NAMES] for i in range(0, 12 * NAMES, NAMES)]
    g, w, m, v, whole, new_m, new_v, slots, theirs, own, m_buf, v_buf = groups
    rs_send, rs_recv, pt_send, pt_recv, own_sem, mv_sem, out_sem, ag_send, ag_recv, pa_send, pa_recv = refs[12 * NAMES :]
    chips = n // CORES
    last = chips - 1
    me = lax.axis_index("dp")
    core, chip = lax.rem(me, CORES), me // CORES
    partner = me + 1 - 2 * core
    up, down = lax.rem(me + CORES, n), lax.rem(me + n - CORES, n)
    to = (up, down)
    pieces = [(d, j) for j in range(NAMES) for d in range(LAYERS)]

    def rows(j, device):
        size = m[j].shape[1]
        return pl.ds(pl.multiple_of(device * size, size), size)

    def rs_chip(d, k):
        return lax.rem(chip + 2 * chips - 1 - k, chips) if d == 0 else lax.rem(chip + 1 + k, chips)

    def ag_chip(d, k):
        return lax.rem(chip + chips - k, chips) if d == 0 else lax.rem(chip + k, chips)

    def remote(src, dst, send, recv, device):
        return pltpu.make_async_remote_copy(src_ref=src, dst_ref=dst, send_sem=send, recv_sem=recv, device_id={"dp": device}, device_id_type=MESH)

    def to_partner(d, j, k):
        block = rows(j, rs_chip(d, k) * CORES + 1 - core)
        return remote(g[j].at[0, d, block], theirs[j].at[d, k], pt_send.at[d, j, k], pt_recv.at[d, j, k], partner)

    def load_own(d, j, k):
        block = rows(j, rs_chip(d, k) * CORES + core)
        half = lax.rem(k, 2)
        return pltpu.make_async_copy(g[j].at[0, d, block], own[j].at[d, half], own_sem.at[d, j, half])

    def load_w(d, j):
        half = (last + 1) % 2
        return pltpu.make_async_copy(w[j].at[d, rows(j, me)], own[j].at[d, half], own_sem.at[d, j, half])

    def ring(d, j, k):
        return remote(slots[j].at[d, k], slots[j].at[d, k + 1], rs_send.at[d, j, k], rs_recv.at[d, j, k + 1], to[d])

    def moments_in(d, j):
        return (
            pltpu.make_async_copy(m[j].at[d], m_buf[j], mv_sem.at[j, 0]),
            pltpu.make_async_copy(v[j].at[d], v_buf[j], mv_sem.at[j, 1]),
        )

    def moments_out(d, j):
        return (
            pltpu.make_async_copy(m_buf[j], new_m[j].at[d], mv_sem.at[j, 2]),
            pltpu.make_async_copy(v_buf[j], new_v[j].at[d], mv_sem.at[j, 3]),
        )

    def pass_on(d, j, k, src, block):
        return remote(src, whole[j].at[d, block], ag_send.at[d, j, k], ag_recv.at[d, j, k + 1], to[d])

    def share(d, j, k, src, block):
        return remote(src, whole[j].at[d, block], pa_send.at[d, j, k], pa_recv.at[d, j, k], partner)

    def keep(d, j):
        return pltpu.make_async_copy(slots[j].at[d, last], whole[j].at[d, rows(j, me)], out_sem.at[d, j])

    barrier = pltpu.get_barrier_semaphore()
    for device in (up, down, partner):
        pl.semaphore_signal(barrier, inc=1, device_id={"dp": device}, device_id_type=MESH)
    for d, j in pieces:
        load_own(d, j, 0).start()
    pl.semaphore_wait(barrier, 3)

    for k in range(2):
        for d, j in pieces:
            to_partner(d, j, k).start()

    def add(d, j, k, first):
        half = lax.rem(k, 2)

        def body(at):
            total = own[j][(d, half, *at)].astype(jnp.float32) + theirs[j][(d, k, *at)].astype(jnp.float32)
            if not first:
                total = total + slots[j][(d, k, *at)].astype(jnp.float32)
            slots[j][(d, k, *at)] = total.astype(jnp.bfloat16)

        chunks(own[j].shape[2:], body)

    def stage(k, first):
        for d, j in pieces:
            load_own(d, j, k + 1).start()
        for d, j in pieces:
            load_own(d, j, k).wait()
            to_partner(d, j, k).wait_recv()
            if not first:
                ring(d, j, k - 1).wait_recv()
            add(d, j, k, first)
            ring(d, j, k).start()

    stage(0, True)

    @pl.loop(1, last)
    def _(k):
        for d, j in pieces:
            to_partner(d, j, k + 1).start()
        stage(k, False)

    for d, j in pieces:
        load_w(d, j).start()
    for d, j in pieces:
        if d == 0:
            for copy in moments_in(d, j):
                copy.start()
    for d, j in pieces:
        load_own(d, j, last).wait()
        to_partner(d, j, last).wait_recv()
        load_w(d, j).wait()
        for copy in moments_in(d, j):
            copy.wait()
        ring(d, j, last - 1).wait_recv()

        def step(at, d=d, j=j):
            total = own[j][(d, last % 2, *at)].astype(jnp.float32) + theirs[j][(d, last, *at)].astype(jnp.float32)
            total = (total + slots[j][(d, last, *at)].astype(jnp.float32)).astype(jnp.bfloat16).astype(jnp.float32)
            new, m_buf[j][at], v_buf[j][at] = adamw(own[j][(d, (last + 1) % 2, *at)].astype(jnp.float32), m_buf[j][at], v_buf[j][at], total)
            slots[j][(d, last, *at)] = new

        chunks(own[j].shape[2:], step)
        for copy in moments_out(d, j):
            copy.start()
        mine = slots[j].at[d, last]
        pass_on(d, j, 0, mine, rows(j, me)).start()
        share(d, j, 0, mine, rows(j, me)).start()
        keep(d, j).start()
        for copy in moments_out(d, j):
            copy.wait()
        if d + 1 < LAYERS:
            for copy in moments_in(d + 1, j):
                copy.start()

    def gather(k, more):
        for d, j in pieces:
            block = rows(j, ag_chip(d, k) * CORES + core)
            here = whole[j].at[d, block]
            pass_on(d, j, k - 1, here, block).wait_recv()
            if more:
                pass_on(d, j, k, here, block).start()
            share(d, j, k, here, block).start()

    @pl.loop(1, last)
    def _(k):
        gather(k, True)

    gather(last, False)

    for d, j in pieces:
        keep(d, j).wait()

    @pl.loop(0, chips)
    def _(k):
        for d, j in pieces:
            block = rows(j, ag_chip(d, k) * CORES + core)
            here = whole[j].at[d, block]
            to_partner(d, j, k).wait_send()
            share(d, j, k, here, block).wait_send()
            share(d, j, k, here, block).wait_recv()

    @pl.loop(0, last)
    def _(k):
        for d, j in pieces:
            block = rows(j, ag_chip(d, k) * CORES + core)
            ring(d, j, k).wait_send()
            pass_on(d, j, k, whole[j].at[d, block], block).wait_send()


def solution(mesh):
    n = mesh.shape["dp"]
    chips = n // CORES

    def step(*arrays):
        terms, weights, m, v = (arrays[i : i + NAMES] for i in range(0, 4 * NAMES, NAMES))
        blocks = [one.shape[1:] for one in m]
        sems = lambda *shape: pltpu.SemaphoreType.DMA(shape)
        full = sems(LAYERS, NAMES, chips)
        any_space = pl.BlockSpec(memory_space=pl.ANY)
        out = pl.pallas_call(
            functools.partial(kernel, n),
            out_shape=[jax.ShapeDtypeStruct(one.shape, one.dtype) for one in (*weights, *m, *v)],
            in_specs=[any_space] * (4 * NAMES),
            out_specs=[any_space] * (3 * NAMES),
            scratch_shapes=[
                *(pltpu.VMEM((LAYERS, chips, *b), jnp.bfloat16) for b in blocks),
                *(pltpu.VMEM((LAYERS, chips, *b), jnp.bfloat16) for b in blocks),
                *(pltpu.VMEM((LAYERS, 2, *b), jnp.bfloat16) for b in blocks),
                *(pltpu.VMEM(b, jnp.float32) for b in blocks),
                *(pltpu.VMEM(b, jnp.float32) for b in blocks),
                full, full, full, full,
                sems(LAYERS, NAMES, 2), sems(NAMES, 4), sems(LAYERS, NAMES),
                full, full, full, full,
            ],
            compiler_params=pltpu.CompilerParams(collective_id=0, has_side_effects=True, vmem_limit_bytes=67_043_328),
            name="step",
        )(*terms, *weights, *m, *v)
        return tuple(out)

    all_of, cut = P(None, None, None), P(None, "dp", None)
    return jax.shard_map(
        step,
        mesh=mesh,
        in_specs=(P(("rep", "dp"), None, None, None),) * 3 + (all_of,) * 3 + (cut,) * 6,
        out_specs=(P("rep", None, None),) * 3 + (P("rep", "dp", None),) * 6,
        check_vma=False,
    )
```

```python
import functools

import jax
import jax.numpy as jnp
from jax import lax
from jax.experimental import pallas as pl
from jax.experimental.pallas import tpu as pltpu
from jax.sharding import PartitionSpec as P

CORES = 2
LAYERS = 2
NAMES = 3
CHUNK = 32768
VMEM_LIMIT = 4_000_000
MESH = pl.DeviceIdType.MESH


def adamw(w, m, v, g):
    m = 0.9 * m + 0.1 * g
    v = 0.95 * v + 0.05 * g * g
    step = m * lax.rsqrt(v + 1e-8) + 0.1 * w
    return (w - 0.02 * step).astype(jnp.bfloat16), m, v


def chunks(shape, body):
    rows, columns = shape
    if columns * rows <= CHUNK:
        body((slice(None), slice(None)))
    elif rows * 128 <= CHUNK and columns % (CHUNK // rows) == 0:
        size = CHUNK // rows

        @pl.loop(0, columns // size)
        def _(i):
            body((slice(None), pl.ds(pl.multiple_of(i * size, size), size)))
    else:
        size = CHUNK // columns

        @pl.loop(0, rows // size)
        def _(i):
            body((pl.ds(pl.multiple_of(i * size, size), size), slice(None)))


def spot(place, at):
    layer, block = place
    row, column = at
    if isinstance(row, slice):
        return layer, block, column
    return layer, pl.ds(pl.multiple_of(block.start + row.start, row.size), row.size), column


def kernel(n, *refs):
    g, w, m, v, whole, new_m, new_v, own = (refs[i : i + NAMES] for i in range(0, 8 * NAMES, NAMES))
    rs_send, rs_recv, pt_send, pt_recv, own_sem, mv_sem, w_sem, ag_send, ag_recv, pa_send, pa_recv, free, pt_free = refs[8 * NAMES :]
    chips = n // CORES
    last = chips - 1
    me = lax.axis_index("dp")
    core, chip = lax.rem(me, CORES), me // CORES
    partner = me + 1 - 2 * core
    up, down = lax.rem(me + CORES, n), lax.rem(me + n - CORES, n)
    to, source = (up, down), (down, up)
    pieces = [(d, j) for j in range(NAMES) for d in range(LAYERS)]

    def rows(j, of_chip, of_core):
        size = m[j].shape[1]
        return pl.ds(pl.multiple_of((of_chip * CORES + of_core) * size, size), size)

    def sum_chip(d, k):
        return lax.rem(chip + 2 * chips - 1 - k, chips) if d == 0 else lax.rem(chip + 1 + k, chips)

    def place(d, j, k):
        return d, rows(j, lax.rem(chip + chips - k, chips) if d == 0 else lax.rem(chip + k, chips), core)

    def their_place(d, j, k):
        return d, rows(j, lax.rem(chip + chips - k, chips) if d == 0 else lax.rem(chip + k, chips), 1 - core)

    def remote(src, dst, send, recv, device):
        return pltpu.make_async_remote_copy(src_ref=src, dst_ref=dst, send_sem=send, recv_sem=recv, device_id={"dp": device}, device_id_type=MESH)

    def to_partner(d, j, k):
        block = rows(j, sum_chip(d, k), 1 - core)
        return remote(g[j].at[0, d, block], whole[j].at[place(d, j, k)], pt_send.at[d, j, k], pt_recv.at[d, j, k], partner)

    def load_own(d, j, k):
        return pltpu.make_async_copy(g[j].at[0, d, rows(j, sum_chip(d, k), core)], own[j].at[d], own_sem.at[d, j])

    def load_w(d, j):
        return pltpu.make_async_copy(w[j].at[d, rows(j, chip, core)], whole[j].at[place(d, j, 0)], w_sem.at[d, j])

    def load_moments(d, j):
        return (
            pltpu.make_async_copy(m[j].at[d], new_m[j].at[d], mv_sem.at[d, j, 0]),
            pltpu.make_async_copy(v[j].at[d], new_v[j].at[d], mv_sem.at[d, j, 1]),
        )

    def ring(d, j, k):
        here = whole[j].at[place(d, j, k)]
        return remote(here, here, rs_send.at[d, j, k], rs_recv.at[d, j, k + 1], to[d])

    def pass_on(d, j, k):
        here = whole[j].at[place(d, j, k)]
        return remote(here, here, ag_send.at[d, j, k], ag_recv.at[d, j, k + 1], to[d])

    def share(d, j, k):
        here = whole[j].at[place(d, j, k)]
        return remote(here, here, pa_send.at[d, j, k], pa_recv.at[d, j, k], partner)

    def allow(d, j, places):
        pl.semaphore_signal(free.at[d, j], inc=places, device_id={"dp": source[d]}, device_id_type=MESH)

    def allow_partner(d, j):
        pl.semaphore_signal(pt_free.at[d, j], inc=1, device_id={"dp": partner}, device_id_type=MESH)

    barrier = pltpu.get_barrier_semaphore()
    for device in (up, down, partner):
        pl.semaphore_signal(barrier, inc=1, device_id={"dp": device}, device_id_type=MESH)
    for d, j in pieces:
        load_own(d, j, 0).start()
    pl.semaphore_wait(barrier, 3)

    def add(d, j, k, first):
        here, there = place(d, j, k), their_place(d, j, k)

        def body(at):
            total = own[j][(d, *at)].astype(jnp.float32) + whole[j][spot(there, at)].astype(jnp.float32)
            if not first:
                total = total + whole[j][spot(here, at)].astype(jnp.float32)
            whole[j][spot(here, at)] = total.astype(jnp.bfloat16)

        chunks(own[j].shape[1:], body)

    def stage(k, first=False, lag=True):
        for d, j in pieces:
            to_partner(d, j, k + 1).start()
        for d, j in pieces:
            load_own(d, j, k).wait()
            to_partner(d, j, k).wait_recv()
            if not first:
                ring(d, j, k - 1).wait_recv()
            add(d, j, k, first)
            load_own(d, j, k + 1).start()
            ring(d, j, k).start()
            allow_partner(d, j)
            if lag:
                ring(d, j, k - 2).wait_send()
                allow(d, j, 1)

    for d, j in pieces:
        to_partner(d, j, 0).start()
    stage(0, first=True, lag=False)
    stage(1, lag=False)
    for d, j in pieces:
        for copy in load_moments(d, j):
            copy.start()

    @pl.loop(2, last)
    def _(k):
        stage(k)

    for d, j in pieces:
        load_w(d, j).start()
    for d, j in pieces:
        load_own(d, j, last).wait()
        to_partner(d, j, last).wait_recv()
        load_w(d, j).wait()
        for copy in load_moments(d, j):
            copy.wait()
        ring(d, j, last - 1).wait_recv()
        mine, here, there = place(d, j, 0), place(d, j, last), their_place(d, j, last)

        def step(at, d=d, j=j, mine=mine, here=here, there=there):
            total = own[j][(d, *at)].astype(jnp.float32) + whole[j][spot(there, at)].astype(jnp.float32)
            total = (total + whole[j][spot(here, at)].astype(jnp.float32)).astype(jnp.bfloat16).astype(jnp.float32)
            new, new_m[j][(d, *at)], new_v[j][(d, *at)] = adamw(
                whole[j][spot(mine, at)].astype(jnp.float32), new_m[j][(d, *at)], new_v[j][(d, *at)], total
            )
            whole[j][spot(mine, at)] = new

        chunks(own[j].shape[1:], step)
        allow_partner(d, j)
        ring(d, j, last - 2).wait_send()
        allow(d, j, 1)
        pl.semaphore_wait(free.at[d, j], 2)
        pass_on(d, j, 0).start()
        pl.semaphore_wait(pt_free.at[d, j], 1)
        share(d, j, 0).start()

    def gather(k, more=True, lag=False):
        for d, j in pieces:
            pass_on(d, j, k - 1).wait_recv()
            if more:
                pl.semaphore_wait(free.at[d, j], 1)
                pass_on(d, j, k).start()
            pl.semaphore_wait(pt_free.at[d, j], 1)
            share(d, j, k).start()
            if lag:
                ring(d, j, last - 1).wait_send()
                allow(d, j, 2)

    gather(1, lag=True)

    @pl.loop(2, last)
    def _(k):
        gather(k)

    gather(last, more=False)

    @pl.loop(0, chips)
    def _(k):
        for d, j in pieces:
            to_partner(d, j, k).wait_send()
            share(d, j, k).wait_send()
            share(d, j, k).wait_recv()

    @pl.loop(0, last)
    def _(k):
        for d, j in pieces:
            pass_on(d, j, k).wait_send()


def finish(*refs):
    count = len(refs[:-1]) // 2
    copies = [pltpu.make_async_copy(refs[i], refs[count + i], refs[-1].at[i]) for i in range(count)]
    for copy in copies:
        copy.start()
    for copy in copies:
        copy.wait()


def solution(mesh):
    n = mesh.shape["dp"]
    chips = n // CORES

    def step(*arrays):
        terms, weights, m, v = (arrays[i : i + NAMES] for i in range(0, 4 * NAMES, NAMES))
        blocks = [one.shape[1:] for one in m]
        sems = lambda *shape: pltpu.SemaphoreType.DMA(shape)
        full = sems(LAYERS, NAMES, chips)
        credits = pltpu.SemaphoreType.REGULAR((LAYERS, NAMES))
        any_space, vmem = (pl.BlockSpec(memory_space=space) for space in (pl.ANY, pltpu.VMEM))
        results = (*weights, *m, *v)
        out = pl.pallas_call(
            functools.partial(kernel, n),
            out_shape=[pltpu.VMEM(one.shape, one.dtype) for one in results],
            in_specs=[any_space] * (4 * NAMES),
            out_specs=[vmem] * (3 * NAMES),
            scratch_shapes=[
                *(pltpu.VMEM((LAYERS, *b), jnp.bfloat16) for b in blocks),
                full, full, full, full,
                sems(LAYERS, NAMES), sems(LAYERS, NAMES, 2), sems(LAYERS, NAMES),
                full, full, full, full,
                credits, credits,
            ],
            compiler_params=pltpu.CompilerParams(collective_id=0, has_side_effects=True, vmem_limit_bytes=VMEM_LIMIT),
            name="step",
        )(*terms, *weights, *m, *v)
        return tuple(
            pl.pallas_call(
                finish,
                out_shape=[jax.ShapeDtypeStruct(one.shape, one.dtype) for one in results],
                in_specs=[vmem] * (3 * NAMES),
                out_specs=[any_space] * (3 * NAMES),
                scratch_shapes=[sems(3 * NAMES)],
                compiler_params=pltpu.CompilerParams(vmem_limit_bytes=VMEM_LIMIT),
                name="finish",
            )(*(pltpu.with_memory_space_constraint(one, pltpu.VMEM) for one in out))
        )

    all_of, cut = P(None, None, None), P(None, "dp", None)
    return jax.shard_map(
        step,
        mesh=mesh,
        in_specs=(P(("rep", "dp"), None, None, None),) * 3 + (all_of,) * 3 + (cut,) * 6,
        out_specs=(P("rep", None, None),) * 3 + (P("rep", "dp", None),) * 6,
        check_vma=False,
    )
```

```python
import functools

import jax
import jax.numpy as jnp
from jax import lax
from jax.experimental import pallas as pl
from jax.experimental.pallas import tpu as pltpu
from jax.sharding import PartitionSpec as P


CORES = 2
LAYERS = 2
NAMES = 3
LATE = (1, 2)
CHUNK = 32768
VMEM_LIMIT = 4_000_000
MESH = pl.DeviceIdType.MESH


def adamw(w, m, v, g):
    m = 0.9 * m + 0.1 * g
    v = 0.95 * v + 0.05 * g * g
    step = m * lax.rsqrt(v + 1e-8) + 0.1 * w
    return (w - 0.02 * step).astype(jnp.bfloat16), m, v


def chunks(shape, body):
    rows, columns = shape
    if columns * rows <= CHUNK:
        body((slice(None), slice(None)))
    elif rows * 128 <= CHUNK and columns % (CHUNK // rows) == 0:
        size = CHUNK // rows

        @pl.loop(0, columns // size)
        def _(i):
            body((slice(None), pl.ds(pl.multiple_of(i * size, size), size)))
    else:
        size = CHUNK // columns

        @pl.loop(0, rows // size)
        def _(i):
            body((pl.ds(pl.multiple_of(i * size, size), size), slice(None)))


def spot(place, at):
    layer, block = place
    row, column = at
    if isinstance(row, slice):
        return layer, block, column
    return layer, pl.ds(pl.multiple_of(block.start + row.start, row.size), row.size), column


def kernel(n, *refs):
    g, w, m, v, whole, new_m, new_v = (refs[i : i + NAMES] for i in range(0, 7 * NAMES, NAMES))
    refs = refs[7 * NAMES :]
    tails, refs = refs[: LAYERS * len(LATE)], refs[LAYERS * len(LATE) :]
    own = refs[:NAMES]
    rs_send, rs_recv, pt_send, pt_recv, own_sem, mv_sem, w_sem, tail_sem, ag_send, ag_recv, pa_send, pa_recv, free, pt_free = refs[NAMES:]
    chips = n // CORES
    last = chips - 1
    me = lax.axis_index("dp")
    core, chip = lax.rem(me, CORES), me // CORES
    partner = me + 1 - 2 * core
    up, down = lax.rem(me + CORES, n), lax.rem(me + n - CORES, n)
    to, source = (up, down), (down, up)
    pieces = [(d, j) for j in range(NAMES) for d in range(LAYERS)]

    def rows(j, of_chip, of_core):
        size = m[j].shape[1]
        return pl.ds(pl.multiple_of((of_chip * CORES + of_core) * size, size), size)

    def sum_chip(d, k):
        return lax.rem(chip + 2 * chips - 1 - k, chips) if d == 0 else lax.rem(chip + 1 + k, chips)

    def place(d, j, k):
        return d, rows(j, lax.rem(chip + chips - k, chips) if d == 0 else lax.rem(chip + k, chips), core)

    def their_place(d, j, k):
        return d, rows(j, lax.rem(chip + chips - k, chips) if d == 0 else lax.rem(chip + k, chips), 1 - core)

    def remote(src, dst, send, recv, device):
        return pltpu.make_async_remote_copy(src_ref=src, dst_ref=dst, send_sem=send, recv_sem=recv, device_id={"dp": device}, device_id_type=MESH)

    def to_partner(d, j, k):
        block = rows(j, sum_chip(d, k), 1 - core)
        return remote(g[j].at[0, d, block], whole[j].at[place(d, j, k)], pt_send.at[d, j, k], pt_recv.at[d, j, k], partner)

    def load_own(d, j, k):
        return pltpu.make_async_copy(g[j].at[0, d, rows(j, sum_chip(d, k), core)], own[j].at[d], own_sem.at[d, j])

    def load_w(d, j):
        return pltpu.make_async_copy(w[j].at[d, rows(j, chip, core)], whole[j].at[place(d, j, 0)], w_sem.at[d, j])

    def load_moments(d, j):
        return (
            pltpu.make_async_copy(m[j].at[d], new_m[j].at[d], mv_sem.at[d, j, 0]),
            pltpu.make_async_copy(v[j].at[d], new_v[j].at[d], mv_sem.at[d, j, 1]),
        )

    def ring(d, j, k):
        here = whole[j].at[place(d, j, k)]
        return remote(here, here, rs_send.at[d, j, k], rs_recv.at[d, j, k + 1], to[d])

    def pass_on(d, j, k):
        here = whole[j].at[place(d, j, k)]
        return remote(here, here, ag_send.at[d, j, k], ag_recv.at[d, j, k + 1], to[d])

    def share(d, j, k):
        here = whole[j].at[place(d, j, k)]
        return remote(here, here, pa_send.at[d, j, k], pa_recv.at[d, j, k], partner)

    def to_tail(d, j):
        at = LATE.index(j) * LAYERS + d
        return pltpu.make_async_copy(whole[j].at[place(d, j, last - 1)], tails[at], tail_sem.at[at])

    def allow(d, j, places):
        pl.semaphore_signal(free.at[d, j], inc=places, device_id={"dp": source[d]}, device_id_type=MESH)

    def allow_partner(d, j):
        pl.semaphore_signal(pt_free.at[d, j], inc=1, device_id={"dp": partner}, device_id_type=MESH)

    barrier = pltpu.get_barrier_semaphore()
    for device in (up, down, partner):
        pl.semaphore_signal(barrier, inc=1, device_id={"dp": device}, device_id_type=MESH)
    for d, j in pieces:
        load_own(d, j, 0).start()
    pl.semaphore_wait(barrier, 3)

    def add(d, j, k, first):
        here, there = place(d, j, k), their_place(d, j, k)

        def body(at):
            total = own[j][(d, *at)].astype(jnp.float32) + whole[j][spot(there, at)].astype(jnp.float32)
            if not first:
                total = total + whole[j][spot(here, at)].astype(jnp.float32)
            whole[j][spot(here, at)] = total.astype(jnp.bfloat16)

        chunks(own[j].shape[1:], body)

    def stage(k, first=False, lag=True):
        for d, j in pieces:
            to_partner(d, j, k + 1).start()
        for d, j in pieces:
            load_own(d, j, k).wait()
            to_partner(d, j, k).wait_recv()
            if not first:
                ring(d, j, k - 1).wait_recv()
            add(d, j, k, first)
            load_own(d, j, k + 1).start()
            ring(d, j, k).start()
            allow_partner(d, j)
            if lag:
                ring(d, j, k - 2).wait_send()
                allow(d, j, 1)

    for d, j in pieces:
        to_partner(d, j, 0).start()
    stage(0, first=True, lag=False)
    stage(1, lag=False)
    for d, j in pieces:
        for copy in load_moments(d, j):
            copy.start()

    @pl.loop(2, last)
    def _(k):
        stage(k)

    for d, j in pieces:
        load_w(d, j).start()
    for d, j in pieces:
        load_own(d, j, last).wait()
        to_partner(d, j, last).wait_recv()
        load_w(d, j).wait()
        for copy in load_moments(d, j):
            copy.wait()
        ring(d, j, last - 1).wait_recv()
        mine, here, there = place(d, j, 0), place(d, j, last), their_place(d, j, last)

        def step(at, d=d, j=j, mine=mine, here=here, there=there):
            total = own[j][(d, *at)].astype(jnp.float32) + whole[j][spot(there, at)].astype(jnp.float32)
            total = (total + whole[j][spot(here, at)].astype(jnp.float32)).astype(jnp.bfloat16).astype(jnp.float32)
            new, new_m[j][(d, *at)], new_v[j][(d, *at)] = adamw(
                whole[j][spot(mine, at)].astype(jnp.float32), new_m[j][(d, *at)], new_v[j][(d, *at)], total
            )
            whole[j][spot(mine, at)] = new

        chunks(own[j].shape[1:], step)
        if j not in LATE:
            allow_partner(d, j)
        ring(d, j, last - 2).wait_send()
        allow(d, j, 1)
        pl.semaphore_wait(free.at[d, j], 2)
        pass_on(d, j, 0).start()
        pl.semaphore_wait(pt_free.at[d, j], 1)
        share(d, j, 0).start()

    def gather(k, lag=False):
        for d, j in pieces:
            pass_on(d, j, k - 1).wait_recv()
            if isinstance(k, int) and k == last - 1 and j in LATE:
                to_tail(d, j).start()
            else:
                pl.semaphore_wait(free.at[d, j], 1)
                pass_on(d, j, k).start()
            pl.semaphore_wait(pt_free.at[d, j], 1)
            share(d, j, k).start()
            if lag:
                ring(d, j, last - 1).wait_send()
                allow(d, j, 1 if j in LATE else 2)

    gather(1, lag=True)

    @pl.loop(2, last - 1)
    def _(k):
        gather(k)

    gather(last - 1)
    for d, j in pieces:
        if j not in LATE:
            pass_on(d, j, last - 1).wait_recv()
            pl.semaphore_wait(pt_free.at[d, j], 1)
            share(d, j, last).start()

    @pl.loop(0, last - 1)
    def _(k):
        for d, j in pieces:
            to_partner(d, j, k).wait_send()
            share(d, j, k).wait_send()
            share(d, j, k).wait_recv()
            pass_on(d, j, k).wait_send()

    for d, j in pieces:
        to_partner(d, j, last - 1).wait_send()
        to_partner(d, j, last).wait_send()
        share(d, j, last - 1).wait_send()
        share(d, j, last - 1).wait_recv()
        if j in LATE:
            to_tail(d, j).wait()
        else:
            pass_on(d, j, last - 1).wait_send()
            share(d, j, last).wait_send()
            share(d, j, last).wait_recv()


def finish(*refs):
    count = len(refs[:-1]) // 2
    copies = [pltpu.make_async_copy(refs[i], refs[count + i], refs[-1].at[i]) for i in range(count)]
    for copy in copies:
        copy.start()
    for copy in copies:
        copy.wait()


def place_late(n, theirs, *refs):
    count = LAYERS * len(LATE)
    late, weights = refs[:count], refs[count + len(LATE) : count + 2 * len(LATE)]
    bufs, sem = refs[count + 2 * len(LATE) : -1], refs[-1]
    chips = n // CORES
    me = lax.axis_index("dp")
    core, chip = lax.rem(me, CORES), me // CORES
    ins, outs = [], []
    for i in range(count):
        d, j = i % LAYERS, i // LAYERS
        size = late[i].shape[0]
        of_chip = lax.rem(chip + (1 if d == 0 else chips - 1), chips)
        block = pl.ds(pl.multiple_of((of_chip * CORES + (1 - core if theirs else core)) * size, size), size)
        if not theirs:
            ins.append(pltpu.make_async_copy(late[i], bufs[i], sem.at[0, i]))
        outs.append(pltpu.make_async_copy(late[i] if theirs else bufs[i], weights[j].at[d, block], sem.at[1, i]))
    for copy in ins:
        copy.start()
    for i in range(count):
        if not theirs:
            ins[i].wait()
        outs[i].start()
    for copy in outs:
        copy.wait()


def solution(mesh):
    n = mesh.shape["dp"]
    chips = n // CORES

    def step(*arrays):
        terms, weights, m, v = (arrays[i : i + NAMES] for i in range(0, 4 * NAMES, NAMES))
        blocks = [one.shape[1:] for one in m]
        sems = lambda *shape: pltpu.SemaphoreType.DMA(shape)
        full = sems(LAYERS, NAMES, chips)
        credits = pltpu.SemaphoreType.REGULAR((LAYERS, NAMES))
        any_space, vmem = (pl.BlockSpec(memory_space=space) for space in (pl.ANY, pltpu.VMEM))
        results = (*weights, *m, *v)
        late = [jax.ShapeDtypeStruct(blocks[j], jnp.bfloat16) for j in LATE for _ in range(LAYERS)]
        out = pl.pallas_call(
            functools.partial(kernel, n),
            out_shape=[pltpu.VMEM(one.shape, one.dtype) for one in results] + late,
            in_specs=[any_space] * (4 * NAMES),
            out_specs=[vmem] * (3 * NAMES) + [any_space] * len(late),
            scratch_shapes=[
                *(pltpu.VMEM((LAYERS, *b), jnp.bfloat16) for b in blocks),
                full, full, full, full,
                sems(LAYERS, NAMES), sems(LAYERS, NAMES, 2), sems(LAYERS, NAMES), sems(len(late)),
                full, full, full, full,
                credits, credits,
            ],
            compiler_params=pltpu.CompilerParams(collective_id=0, has_side_effects=True, vmem_limit_bytes=VMEM_LIMIT),
            name="step",
        )(*terms, *weights, *m, *v)
        hop = [[(i, (i + CORES) % n) for i in range(n)], [(i, (i - CORES) % n) for i in range(n)]]
        come = []
        for i, one in enumerate(out[3 * NAMES :]):
            come.append(lax.ppermute(one, "dp", hop[i % LAYERS]))
        across = []
        for one in come:
            across.append(lax.ppermute(one, "dp", [(i, i + 1 - 2 * (i % CORES)) for i in range(n)]))
        done = pl.pallas_call(
            finish,
            out_shape=[jax.ShapeDtypeStruct(one.shape, one.dtype) for one in results],
            in_specs=[vmem] * (3 * NAMES),
            out_specs=[any_space] * (3 * NAMES),
            scratch_shapes=[sems(3 * NAMES)],
            compiler_params=pltpu.CompilerParams(vmem_limit_bytes=VMEM_LIMIT),
            cost_estimate=pl.CostEstimate(flops=20_000_000_000, bytes_accessed=64_000_000, transcendentals=0),
            name="finish",
        )(*(pltpu.with_memory_space_constraint(one, pltpu.VMEM) for one in out[: 3 * NAMES]))
        done = list(done)
        for theirs, blocks_late, space in ((False, come, pltpu.HBM), (True, across, pltpu.VMEM)):
            placed = pl.pallas_call(
                functools.partial(place_late, n, theirs),
                out_shape=[jax.ShapeDtypeStruct(done[j].shape, done[j].dtype) for j in LATE],
                in_specs=[vmem if theirs else any_space] * len(late) + [any_space] * len(LATE),
                out_specs=[any_space] * len(LATE),
                scratch_shapes=[*([] if theirs else [pltpu.VMEM(one.shape, one.dtype) for one in late]), sems(2, len(late))],
                input_output_aliases={len(late) + i: i for i in range(len(LATE))},
                compiler_params=pltpu.CompilerParams(vmem_limit_bytes=VMEM_LIMIT),
            )(*(pltpu.with_memory_space_constraint(one, space) for one in blocks_late), *(done[j] for j in LATE))
            for j, one in zip(LATE, placed, strict=True):
                done[j] = one
        return tuple(done)

    all_of, cut = P(None, None, None), P(None, "dp", None)
    return jax.shard_map(
        step,
        mesh=mesh,
        in_specs=(P(("rep", "dp"), None, None, None),) * 3 + (all_of,) * 3 + (cut,) * 6,
        out_specs=(P("rep", None, None),) * 3 + (P("rep", "dp", None),) * 6,
        check_vma=False,
    )
```

```python
import functools

import jax
import jax.numpy as jnp
from jax import lax
from jax.experimental import pallas as pl
from jax.experimental.pallas import tpu as pltpu
from jax.sharding import PartitionSpec as P


CORES = 2
LAYERS = 2
NAMES = 3
ORDER = (2, 0, 1)
LATE = (0, 1)
END = ORDER[0]
SPLIT = 1
FIRST = 4
CHUNK = 32768
VMEM_LIMIT = 4_000_000
MESH = pl.DeviceIdType.MESH


def adamw(w, m, v, g):
    m = 0.9 * m + 0.1 * g
    v = 0.95 * v + 0.05 * g * g
    step = m * lax.rsqrt(v + 1e-8) + 0.1 * w
    return (w - 0.02 * step).astype(jnp.bfloat16), m, v


def chunks(shape, body):
    rows, columns = shape
    if columns * 16 <= CHUNK:
        size = min(rows, CHUNK // columns)

        @pl.loop(0, rows // size)
        def _(i):
            body((pl.ds(pl.multiple_of(i * size, size), size), slice(None)))
    else:
        size = min(columns, CHUNK // rows)

        @pl.loop(0, columns // size)
        def _(i):
            body((slice(None), pl.ds(pl.multiple_of(i * size, size), size)))


def spot(place, at):
    layer, block = place
    row, column = at
    if isinstance(row, slice):
        return layer, block, column
    return layer, pl.ds(pl.multiple_of(block.start + row.start, row.size), row.size), column


def kernel(n, *refs):
    g, w, m, v, whole, new_m, new_v = (refs[i : i + NAMES] for i in range(0, 7 * NAMES, NAMES))
    refs = refs[7 * NAMES :]
    tails, end, own, sems = refs[:LAYERS], refs[LAYERS], refs[LAYERS + 1 : LAYERS + 1 + NAMES], refs[LAYERS + 1 + NAMES :]
    rs_send, rs_recv, pt_send, pt_recv, first_recv, own_sem, m_sem, v_sem, w_sem, tail_sem, ag_send, ag_recv, pa_send, pa_recv, free, pt_free = sems
    chips = n // CORES
    last = chips - 1
    me = lax.axis_index("dp")
    core, chip = lax.rem(me, CORES), me // CORES
    partner = me + 1 - 2 * core
    up, down = lax.rem(me + CORES, n), lax.rem(me + n - CORES, n)
    to, source = (up, down), (down, up)
    pieces = [(d, (j, h)) for j in ORDER for h in range(SPLIT) for d in range(LAYERS)]

    def sem(array, d, p, *k):
        return array.at[(d, p[0] * SPLIT + p[1], *k)]

    def part(p):
        size = m[p[0]].shape[1] // SPLIT
        return pl.ds(p[1] * size, size)

    def rows(p, of_chip, of_core):
        j, h = p
        block = m[j].shape[1]
        size = block // SPLIT
        return pl.ds(pl.multiple_of((of_chip * CORES + of_core) * block + h * size, size), size)

    def sum_chip(d, k):
        return lax.rem(chip + 2 * chips - 1 - k, chips) if d == 0 else lax.rem(chip + 1 + k, chips)

    def place_chip(d, k):
        return lax.rem(chip + chips - k, chips) if d == 0 else lax.rem(chip + k, chips)

    def place(d, p, k):
        return d, rows(p, place_chip(d, k), core)

    def their_place(d, p, k):
        return d, rows(p, place_chip(d, k), 1 - core)

    def remote(src, dst, send, recv, device):
        return pltpu.make_async_remote_copy(src_ref=src, dst_ref=dst, send_sem=send, recv_sem=recv, device_id={"dp": device}, device_id_type=MESH)

    def to_partner(d, p, k):
        mine = g[p[0]].at[0, d, rows(p, sum_chip(d, k), 1 - core)]
        return remote(mine, whole[p[0]].at[place(d, p, k)], sem(pt_send, d, p, k), sem(pt_recv, d, p, k), partner)

    def quarter(block, s):
        size = block.size // FIRST
        return pl.ds(pl.multiple_of(block.start + s * size, size), size)

    def first_to_partner(d, p, s):
        j = p[0]
        mine = g[j].at[0, d, quarter(rows(p, sum_chip(d, 0), 1 - core), s)]
        there = whole[j].at[d, quarter(place(d, p, 0)[1], s)]
        return remote(mine, there, sem(pt_send, d, p, 0), first_recv.at[d, s], partner)

    def first_ring(d, p, s):
        here = whole[p[0]].at[d, quarter(place(d, p, 0)[1], s)]
        return remote(here, here, sem(rs_send, d, p, 0), sem(rs_recv, d, p, 1), to[d])

    def load_own(d, p, k):
        return pltpu.make_async_copy(g[p[0]].at[0, d, rows(p, sum_chip(d, k), core)], own[p[0]].at[d, part(p)], sem(own_sem, d, p))

    def load_w(d, p):
        return pltpu.make_async_copy(w[p[0]].at[d, rows(p, chip, core)], whole[p[0]].at[place(d, p, 0)], sem(w_sem, d, p))

    def load_moments(d, p):
        return (
            pltpu.make_async_copy(m[p[0]].at[d, part(p)], new_m[p[0]].at[d, part(p)], sem(m_sem, d, p)),
            pltpu.make_async_copy(v[p[0]].at[d, part(p)], new_v[p[0]].at[d, part(p)], sem(v_sem, d, p)),
        )

    def ring(d, p, k):
        here = whole[p[0]].at[place(d, p, k)]
        return remote(here, here, sem(rs_send, d, p, k), sem(rs_recv, d, p, k + 1), to[d])

    def pass_on(d, p, k):
        here = whole[p[0]].at[place(d, p, k)]
        return remote(here, here, sem(ag_send, d, p, k), sem(ag_recv, d, p, k + 1), to[d])

    def share(d, p, k):
        here = whole[p[0]].at[place(d, p, k)]
        return remote(here, here, sem(pa_send, d, p, k), sem(pa_recv, d, p, k), partner)

    def to_tail(d, p):
        return pltpu.make_async_copy(whole[p[0]].at[place(d, p, last - 1)], tails[d].at[LATE.index(p[0]), part(p)], sem(tail_sem, d, p))

    def last_hop(d, p):
        return remote(whole[p[0]].at[place(d, p, last - 1)], end.at[d, part(p)], sem(ag_send, d, p, last - 1), sem(ag_recv, d, p, last), to[d])

    def allow(d, p, places):
        pl.semaphore_signal(sem(free, d, p), inc=places, device_id={"dp": source[d]}, device_id_type=MESH)

    def allow_partner(d, p):
        pl.semaphore_signal(sem(pt_free, d, p), inc=1, device_id={"dp": partner}, device_id_type=MESH)

    barrier = pltpu.get_barrier_semaphore()
    for device in (up, down, partner):
        pl.semaphore_signal(barrier, inc=1, device_id={"dp": device}, device_id_type=MESH)
    for d, p in pieces:
        load_own(d, p, 0).start()
    pl.semaphore_wait(barrier, 3)

    def add(d, p, k, first, s=None):
        j = p[0]
        here, there, mine = place(d, p, k), their_place(d, p, k), (d, part(p))
        if s is not None:
            here, there, mine = ((layer, quarter(block, s)) for layer, block in (here, there, mine))

        def body(at):
            total = own[j][spot(mine, at)].astype(jnp.float32) + whole[j][spot(there, at)].astype(jnp.float32)
            if not first:
                total = total + whole[j][spot(here, at)].astype(jnp.float32)
            whole[j][spot(here, at)] = total.astype(jnp.bfloat16)

        chunks((here[1].size, own[j].shape[2]), body)

    def stage(k, first=False, lag=True):
        if not first:
            for d, p in pieces:
                to_partner(d, p, k + 1).start()
        for d, p in pieces[LAYERS:] if first else pieces:
            load_own(d, p, k).wait()
            to_partner(d, p, k).wait_recv()
            if not first:
                ring(d, p, k - 1).wait_recv()
            add(d, p, k, first)
            load_own(d, p, k + 1).start()
            ring(d, p, k).start()
            allow_partner(d, p)
            if lag:
                ring(d, p, k - 2).wait_send()
                allow(d, p, 1)

    for s in range(FIRST):
        for d, p in pieces[:LAYERS]:
            first_to_partner(d, p, s).start()
    for k in range(2):
        for d, p in pieces[LAYERS:] if k == 0 else pieces:
            to_partner(d, p, k).start()
    for s in range(FIRST):
        for d, p in pieces[:LAYERS]:
            if s == 0:
                load_own(d, p, 0).wait()
            first_to_partner(d, p, s).wait_recv()
            add(d, p, 0, True, s)
            first_ring(d, p, s).start()
    for d, p in pieces[:LAYERS]:
        load_own(d, p, 1).start()
        allow_partner(d, p)
    stage(0, first=True, lag=False)
    stage(1, lag=False)
    for d, p in pieces:
        for copy in load_moments(d, p):
            copy.start()

    @pl.loop(2, last)
    def _(k):
        stage(k)

    for d, p in pieces:
        load_w(d, p).start()
    for d, p in pieces:
        j = p[0]
        load_own(d, p, last).wait()
        to_partner(d, p, last).wait_recv()
        load_w(d, p).wait()
        for copy in load_moments(d, p):
            copy.wait()
        ring(d, p, last - 1).wait_recv()
        mine, here, there, block = place(d, p, 0), place(d, p, last), their_place(d, p, last), (d, part(p))

        def step(at, j=j, mine=mine, here=here, there=there, block=block):
            total = own[j][spot(block, at)].astype(jnp.float32) + whole[j][spot(there, at)].astype(jnp.float32)
            total = (total + whole[j][spot(here, at)].astype(jnp.float32)).astype(jnp.bfloat16).astype(jnp.float32)
            new, new_m[j][spot(block, at)], new_v[j][spot(block, at)] = adamw(
                whole[j][spot(mine, at)].astype(jnp.float32), new_m[j][spot(block, at)], new_v[j][spot(block, at)], total
            )
            whole[j][spot(mine, at)] = new

        chunks((here[1].size, own[j].shape[2]), step)
        ring(d, p, last - 2).wait_send()
        allow(d, p, 1)
        pl.semaphore_wait(sem(free, d, p), 2)
        pass_on(d, p, 0).start()
        pl.semaphore_wait(sem(pt_free, d, p), 1)
        share(d, p, 0).start()

    def gather(k, lag=False, final=False):
        for d, p in pieces:
            pass_on(d, p, k - 1).wait_recv()
            if final and p[0] == END:
                last_hop(d, p).start()
            elif final:
                to_tail(d, p).start()
            else:
                pl.semaphore_wait(sem(free, d, p), 1)
                pass_on(d, p, k).start()
            pl.semaphore_wait(sem(pt_free, d, p), 1)
            share(d, p, k).start()
            if lag:
                ring(d, p, last - 1).wait_send()
                allow(d, p, 1)

    gather(1, lag=True)

    @pl.loop(2, last - 1)
    def _(k):
        gather(k)

    gather(last - 1, final=True)

    @pl.loop(0, last - 1)
    def _(k):
        for d, p in pieces:
            to_partner(d, p, k).wait_send()
            share(d, p, k).wait_send()
            share(d, p, k).wait_recv()
            pass_on(d, p, k).wait_send()

    for d, p in pieces:
        to_partner(d, p, last - 1).wait_send()
        to_partner(d, p, last).wait_send()
        share(d, p, last - 1).wait_send()
        share(d, p, last - 1).wait_recv()
        if p[0] in LATE:
            to_tail(d, p).wait()
    for d, p in pieces:
        if p[0] == END:
            last_hop(d, p).wait_send()
            last_hop(d, p).wait_recv()


def finish(n, *refs):
    count = (len(refs) - 1) // 2
    ins, outs, sem = refs[:count], refs[count : 2 * count], refs[-1]
    chips = n // CORES
    chip = lax.axis_index("dp") // CORES
    copies = []
    for j in range(count):
        for d in range(LAYERS):
            if j < NAMES:
                size = ins[j].shape[1] // chips
                for k in range(chips - 1):
                    at = d, pl.ds(pl.multiple_of(lax.rem(chip + (chips - k if d == 0 else k), chips) * size, size), size)
                    copies.append((ins[j].at[at], outs[j].at[at]))
            else:
                copies.append((ins[j].at[d], outs[j].at[d]))
    copies = [pltpu.make_async_copy(*one, sem.at[i]) for i, one in enumerate(copies)]
    for copy in copies:
        copy.start()
    for copy in copies:
        copy.wait()


def place_late(n, items, arrays, weights, *refs):
    late, out = refs[:arrays], refs[arrays + weights : arrays + 2 * weights]
    bufs, sem = refs[arrays + 2 * weights : -1], refs[-1]
    chips = n // CORES
    me = lax.axis_index("dp")
    core, chip = lax.rem(me, CORES), me // CORES
    ins, outs = [], []
    for x, (array, i, theirs, weight, d) in enumerate(items):
        size = late[array].shape[1]
        of_chip = lax.rem(chip + (1 if d == 0 else chips - 1), chips)
        block = pl.ds(pl.multiple_of((of_chip * CORES + (1 - core if theirs else core)) * size, size), size)
        if bufs:
            ins.append(pltpu.make_async_copy(late[array].at[i], bufs[0].at[x], sem.at[0, x]))
        outs.append(pltpu.make_async_copy(bufs[0].at[x] if bufs else late[array].at[i], out[weight].at[d, block], sem.at[1, x]))
    for copy in ins:
        copy.start()
    for x, copy in enumerate(outs):
        if bufs:
            ins[x].wait()
        copy.start()
    for copy in outs:
        copy.wait()


def solution(mesh):
    n = mesh.shape["dp"]
    chips = n // CORES

    def step(*arrays):
        terms, weights, m, v = (arrays[i : i + NAMES] for i in range(0, 4 * NAMES, NAMES))
        blocks = [one.shape[1:] for one in m]
        sems = lambda *shape: pltpu.SemaphoreType.DMA(shape)
        one_each, full = sems(LAYERS, NAMES * SPLIT), sems(LAYERS, NAMES * SPLIT, chips)
        credits = pltpu.SemaphoreType.REGULAR((LAYERS, NAMES * SPLIT))
        any_space, vmem = (pl.BlockSpec(memory_space=space) for space in (pl.ANY, pltpu.VMEM))
        results = (*weights, *m, *v)
        late = [jax.ShapeDtypeStruct((len(LATE), *blocks[LATE[0]]), jnp.bfloat16)] * LAYERS
        late.append(jax.ShapeDtypeStruct((LAYERS, *blocks[END]), jnp.bfloat16))
        out = pl.pallas_call(
            functools.partial(kernel, n),
            out_shape=[pltpu.VMEM(one.shape, one.dtype) for one in results] + late,
            in_specs=[any_space] * (4 * NAMES),
            out_specs=[vmem] * (3 * NAMES) + [any_space] * len(late),
            scratch_shapes=[
                *(pltpu.VMEM((LAYERS, *b), jnp.bfloat16) for b in blocks),
                full, full, full, full,
                sems(LAYERS, FIRST), one_each, one_each, one_each, one_each, one_each,
                full, full, full, full,
                credits, credits,
            ],
            compiler_params=pltpu.CompilerParams(collective_id=0, has_side_effects=True, vmem_limit_bytes=VMEM_LIMIT),
            name="step",
        )(*terms, *weights, *m, *v)

        def hop(i, one):
            by = CORES if i == 0 else n - CORES
            return lax.ppermute(one, "dp", [(a, (a + by) % n) for a in range(n)])

        def across(one):
            return lax.ppermute(one, "dp", [(a, a + 1 - 2 * (a % CORES)) for a in range(n)])

        *tails, end = out[3 * NAMES :]
        come = [hop(i, one) for i, one in enumerate(tails)]
        ends = [end, across(end)]
        shared = [across(one) for one in come]
        done = pl.pallas_call(
            functools.partial(finish, n),
            out_shape=[jax.ShapeDtypeStruct(one.shape, one.dtype) for one in results],
            in_specs=[vmem] * (3 * NAMES),
            out_specs=[any_space] * (3 * NAMES),
            scratch_shapes=[sems(LAYERS * NAMES * (chips + 1))],
            compiler_params=pltpu.CompilerParams(vmem_limit_bytes=VMEM_LIMIT),
            cost_estimate=pl.CostEstimate(flops=20_000_000_000, bytes_accessed=64_000_000, transcendentals=0),
            name="finish",
        )(*(pltpu.with_memory_space_constraint(one, pltpu.VMEM) for one in out[: 3 * NAMES]))
        done = list(done)

        def place(js, sources, space, items):
            blocks_late = [pltpu.with_memory_space_constraint(one, space) for one in sources]
            bounce = [pltpu.VMEM((len(items), *sources[0].shape[1:]), jnp.bfloat16)] if space is pltpu.HBM else []
            placed = pl.pallas_call(
                functools.partial(place_late, n, items, len(sources), len(js)),
                out_shape=[jax.ShapeDtypeStruct(done[j].shape, done[j].dtype) for j in js],
                in_specs=[any_space if bounce else vmem] * len(sources) + [any_space] * len(js),
                out_specs=[any_space] * len(js),
                scratch_shapes=[*bounce, sems(2, len(items))],
                input_output_aliases={len(sources) + i: i for i in range(len(js))},
                compiler_params=pltpu.CompilerParams(vmem_limit_bytes=VMEM_LIMIT),
            )(*blocks_late, *(done[j] for j in js))
            for j, one in zip(js, placed, strict=True):
                done[j] = one

        place((END,), ends, pltpu.HBM, [(i, d, i == 1, 0, d) for i in range(2) for d in range(LAYERS)])
        place(LATE, come, pltpu.HBM, [(d, i, False, i, d) for i in range(len(LATE)) for d in range(LAYERS)])
        place(LATE, shared, pltpu.VMEM, [(d, i, True, i, d) for i in range(len(LATE)) for d in range(LAYERS)])
        return tuple(done)

    all_of, cut = P(None, None, None), P(None, "dp", None)
    return jax.shard_map(
        step,
        mesh=mesh,
        in_specs=(P(("rep", "dp"), None, None, None),) * 3 + (all_of,) * 3 + (cut,) * 6,
        out_specs=(P("rep", None, None),) * 3 + (P("rep", "dp", None),) * 6,
        check_vma=False,
    )
```

```python
import functools

import jax
import jax.numpy as jnp
from jax import lax
from jax.experimental import pallas as pl
from jax.experimental.pallas import tpu as pltpu
from jax.sharding import PartitionSpec as P


CORES = 2
LAYERS = 2
NAMES = 3
LATE = (0, 1)
END = 2
PIECES = ((0, END), (1, END), (0, LATE[0]), (1, LATE[1]))
FIRST = 8
CHUNK = 32768
VMEM_LIMIT = 4_000_000
MESH = pl.DeviceIdType.MESH


def adamw(w, m, v, g):
    m = 0.9 * m + 0.1 * g
    v = 0.95 * v + 0.05 * g * g
    step = m * lax.rsqrt(v + 1e-8) + 0.1 * w
    return (w - 0.02 * step).astype(jnp.bfloat16), m, v


def chunks(shape, body):
    rows, columns = shape
    if columns * 16 <= CHUNK:
        size = min(rows, CHUNK // columns)

        @pl.loop(0, rows // size)
        def _(i):
            body((pl.ds(pl.multiple_of(i * size, size), size), slice(None)))
    else:
        size = min(columns, CHUNK // rows)

        @pl.loop(0, columns // size)
        def _(i):
            body((slice(None), pl.ds(pl.multiple_of(i * size, size), size)))


def spot(place, at):
    layer, block = place
    row, column = at
    if isinstance(row, slice):
        return layer, block, column
    return layer, pl.ds(pl.multiple_of(block.start + row.start, row.size), row.size), column


def layers(d, j):
    return (d,) if j == END else tuple(range(LAYERS))


def kernel(n, *refs):
    g, w, m, v, whole, new_m, new_v = (refs[i : i + NAMES] for i in range(0, 7 * NAMES, NAMES))
    refs = refs[7 * NAMES :]
    tails, end, own, sems = refs[:LAYERS], refs[LAYERS], refs[LAYERS + 1 : LAYERS + 1 + NAMES], refs[LAYERS + 1 + NAMES :]
    rs_send, rs_recv, pt_send, pt_recv, first_recv, own_sem, m_sem, v_sem, w_sem, tail_sem, ag_send, ag_recv, pa_send, pa_recv, free, pt_free = sems
    chips = n // CORES
    last = chips - 1
    me = lax.axis_index("dp")
    core, chip = lax.rem(me, CORES), me // CORES
    partner = me + 1 - 2 * core
    up, down = lax.rem(me + CORES, n), lax.rem(me + n - CORES, n)
    to, source = (up, down), (down, up)

    def sem(array, d, j, *k):
        return array.at[(d, 0 if j == END else 1, *k)]

    def span(d, j):
        return pl.ds(layers(d, j)[0], len(layers(d, j)))

    def rows(j, of_chip, of_core):
        size = m[j].shape[1]
        return pl.ds(pl.multiple_of((of_chip * CORES + of_core) * size, size), size)

    def sum_chip(d, k):
        return lax.rem(chip + 2 * chips - 1 - k, chips) if d == 0 else lax.rem(chip + 1 + k, chips)

    def place_chip(d, k):
        return lax.rem(chip + chips - k, chips) if d == 0 else lax.rem(chip + k, chips)

    def place(d, j, k):
        return rows(j, place_chip(d, k), core)

    def their_place(d, j, k):
        return rows(j, place_chip(d, k), 1 - core)

    def remote(src, dst, send, recv, device):
        return pltpu.make_async_remote_copy(src_ref=src, dst_ref=dst, send_sem=send, recv_sem=recv, device_id={"dp": device}, device_id_type=MESH)

    def to_partner(d, j, k):
        mine = g[j].at[0, span(d, j), rows(j, sum_chip(d, k), 1 - core)]
        return remote(mine, whole[j].at[span(d, j), place(d, j, k)], sem(pt_send, d, j, k), sem(pt_recv, d, j, k), partner)

    def quarter(block, s):
        size = block.size // FIRST
        return pl.ds(pl.multiple_of(block.start + s * size, size), size)

    def first_to_partner(d, j, s):
        mine = g[j].at[0, span(d, j), quarter(rows(j, sum_chip(d, 0), 1 - core), s)]
        there = whole[j].at[span(d, j), quarter(place(d, j, 0), s)]
        return remote(mine, there, sem(pt_send, d, j, 0), first_recv.at[d, s], partner)

    def first_ring(d, j, s):
        here = whole[j].at[span(d, j), quarter(place(d, j, 0), s)]
        return remote(here, here, sem(rs_send, d, j, 0), sem(rs_recv, d, j, 1), to[d])

    def load_own(d, j, k):
        return pltpu.make_async_copy(g[j].at[0, span(d, j), rows(j, sum_chip(d, k), core)], own[j].at[span(d, j)], sem(own_sem, d, j))

    def load_w(d, j):
        return pltpu.make_async_copy(w[j].at[span(d, j), rows(j, chip, core)], whole[j].at[span(d, j), place(d, j, 0)], sem(w_sem, d, j))

    def load_moments(d, j):
        return (
            pltpu.make_async_copy(m[j].at[span(d, j)], new_m[j].at[span(d, j)], sem(m_sem, d, j)),
            pltpu.make_async_copy(v[j].at[span(d, j)], new_v[j].at[span(d, j)], sem(v_sem, d, j)),
        )

    def ring(d, j, k):
        here = whole[j].at[span(d, j), place(d, j, k)]
        return remote(here, here, sem(rs_send, d, j, k), sem(rs_recv, d, j, k + 1), to[d])

    def pass_on(d, j, k):
        here = whole[j].at[span(d, j), place(d, j, k)]
        return remote(here, here, sem(ag_send, d, j, k), sem(ag_recv, d, j, k + 1), to[d])

    def share(d, j, k):
        here = whole[j].at[span(d, j), place(d, j, k)]
        return remote(here, here, sem(pa_send, d, j, k), sem(pa_recv, d, j, k), partner)

    def to_tail(d, j):
        return pltpu.make_async_copy(whole[j].at[span(d, j), place(d, j, last - 1)], tails[d], tail_sem.at[d])

    def last_hop(d, j):
        here = whole[j].at[span(d, j), place(d, j, last - 1)]
        return remote(here, end.at[span(d, j)], sem(ag_send, d, j, last - 1), sem(ag_recv, d, j, last), to[d])

    def allow(d, j, places):
        pl.semaphore_signal(sem(free, d, j), inc=places, device_id={"dp": source[d]}, device_id_type=MESH)

    def allow_partner(d, j):
        pl.semaphore_signal(sem(pt_free, d, j), inc=1, device_id={"dp": partner}, device_id_type=MESH)

    barrier = pltpu.get_barrier_semaphore()
    for device in (up, down, partner):
        pl.semaphore_signal(barrier, inc=1, device_id={"dp": device}, device_id_type=MESH)
    for d, j in PIECES:
        load_own(d, j, 0).start()
    pl.semaphore_wait(barrier, 3)

    def add(d, j, k, first, s=None):
        here, there, mine = place(d, j, k), their_place(d, j, k), pl.ds(0, own[j].shape[1])
        if s is not None:
            here, there, mine = (quarter(block, s) for block in (here, there, mine))
        for layer in layers(d, j):

            def body(at, layer=layer):
                total = own[j][spot((layer, mine), at)].astype(jnp.float32) + whole[j][spot((layer, there), at)].astype(jnp.float32)
                if not first:
                    total = total + whole[j][spot((layer, here), at)].astype(jnp.float32)
                whole[j][spot((layer, here), at)] = total.astype(jnp.bfloat16)

            chunks((here.size, own[j].shape[2]), body)

    def stage(k, first=False, lag=True):
        if not first:
            for d, j in PIECES:
                to_partner(d, j, k + 1).start()
        for d, j in PIECES[LAYERS:] if first else PIECES:
            load_own(d, j, k).wait()
            to_partner(d, j, k).wait_recv()
            if not first:
                ring(d, j, k - 1).wait_recv()
            add(d, j, k, first)
            load_own(d, j, k + 1).start()
            ring(d, j, k).start()
            allow_partner(d, j)
            if lag:
                ring(d, j, k - 2).wait_send()
                allow(d, j, 1)

    for s in range(FIRST):
        for d, j in PIECES[:LAYERS]:
            first_to_partner(d, j, s).start()
    for k in range(2):
        for d, j in PIECES[LAYERS:] if k == 0 else PIECES:
            to_partner(d, j, k).start()
    for s in range(FIRST):
        for d, j in PIECES[:LAYERS]:
            if s == 0:
                load_own(d, j, 0).wait()
            first_to_partner(d, j, s).wait_recv()
            add(d, j, 0, True, s)
            first_ring(d, j, s).start()
    for d, j in PIECES[:LAYERS]:
        load_own(d, j, 1).start()
        allow_partner(d, j)
    stage(0, first=True, lag=False)
    stage(1, lag=False)
    for d, j in PIECES:
        for copy in load_moments(d, j):
            copy.start()

    @pl.loop(2, last)
    def _(k):
        stage(k)

    for d, j in PIECES:
        load_w(d, j).start()
    for d, j in PIECES:
        load_own(d, j, last).wait()
        to_partner(d, j, last).wait_recv()
        load_w(d, j).wait()
        for copy in load_moments(d, j):
            copy.wait()
        ring(d, j, last - 1).wait_recv()
        mine, here, there, block = place(d, j, 0), place(d, j, last), their_place(d, j, last), pl.ds(0, own[j].shape[1])
        for layer in layers(d, j):

            def step(at, j=j, layer=layer, mine=mine, here=here, there=there, block=block):
                own_at = spot((layer, block), at)
                total = own[j][own_at].astype(jnp.float32) + whole[j][spot((layer, there), at)].astype(jnp.float32)
                total = (total + whole[j][spot((layer, here), at)].astype(jnp.float32)).astype(jnp.bfloat16).astype(jnp.float32)
                old = whole[j][spot((layer, mine), at)].astype(jnp.float32)
                new, new_m[j][own_at], new_v[j][own_at] = adamw(old, new_m[j][own_at], new_v[j][own_at], total)
                whole[j][spot((layer, mine), at)] = new

            chunks((here.size, own[j].shape[2]), step)
        ring(d, j, last - 2).wait_send()
        allow(d, j, 1)
        pl.semaphore_wait(sem(free, d, j), 2)
        pass_on(d, j, 0).start()
        pl.semaphore_wait(sem(pt_free, d, j), 1)
        share(d, j, 0).start()

    def gather(k, lag=False, final=False):
        for d, j in PIECES:
            pass_on(d, j, k - 1).wait_recv()
            if final and j == END:
                last_hop(d, j).start()
            elif final:
                to_tail(d, j).start()
            else:
                pl.semaphore_wait(sem(free, d, j), 1)
                pass_on(d, j, k).start()
            pl.semaphore_wait(sem(pt_free, d, j), 1)
            share(d, j, k).start()
            if lag:
                ring(d, j, last - 1).wait_send()
                allow(d, j, 1)

    gather(1, lag=True)

    @pl.loop(2, last - 1)
    def _(k):
        gather(k)

    gather(last - 1, final=True)

    @pl.loop(0, last - 1)
    def _(k):
        for d, j in PIECES:
            to_partner(d, j, k).wait_send()
            share(d, j, k).wait_send()
            share(d, j, k).wait_recv()
            pass_on(d, j, k).wait_send()

    for d, j in PIECES:
        to_partner(d, j, last - 1).wait_send()
        to_partner(d, j, last).wait_send()
        share(d, j, last - 1).wait_send()
        share(d, j, last - 1).wait_recv()
        if j in LATE:
            to_tail(d, j).wait()
    for d, j in PIECES:
        if j == END:
            last_hop(d, j).wait_send()
            last_hop(d, j).wait_recv()


def finish(n, *refs):
    count = (len(refs) - 1) // 2
    ins, outs, sem = refs[:count], refs[count : 2 * count], refs[-1]
    chips = n // CORES
    chip = lax.axis_index("dp") // CORES
    copies = []
    for j in range(count):
        for d in range(LAYERS):
            if j < NAMES:
                size = ins[j].shape[1] // chips
                for k in range(chips - 1):
                    up = (d if j == END else LATE.index(j)) == 0
                    at = d, pl.ds(pl.multiple_of(lax.rem(chip + (chips - k if up else k), chips) * size, size), size)
                    copies.append((ins[j].at[at], outs[j].at[at]))
            else:
                copies.append((ins[j].at[d], outs[j].at[d]))
    copies = [pltpu.make_async_copy(*one, sem.at[i]) for i, one in enumerate(copies)]
    for copy in copies:
        copy.start()
    for copy in copies:
        copy.wait()


def place_late(n, items, arrays, weights, *refs):
    late, out = refs[:arrays], refs[arrays + weights : arrays + 2 * weights]
    bufs, sem = refs[arrays + 2 * weights : -1], refs[-1]
    chips = n // CORES
    me = lax.axis_index("dp")
    core, chip = lax.rem(me, CORES), me // CORES
    ins, outs = [], []
    for x, (array, layer, theirs, weight, d) in enumerate(items):
        size = late[array].shape[1]
        of_chip = lax.rem(chip + (1 if d == 0 else chips - 1), chips)
        block = pl.ds(pl.multiple_of((of_chip * CORES + (1 - core if theirs else core)) * size, size), size)
        if bufs:
            ins.append(pltpu.make_async_copy(late[array].at[layer], bufs[0].at[x], sem.at[0, x]))
        outs.append(pltpu.make_async_copy(bufs[0].at[x] if bufs else late[array].at[layer], out[weight].at[layer, block], sem.at[1, x]))
    for copy in ins:
        copy.start()
    for x, copy in enumerate(outs):
        if bufs:
            ins[x].wait()
        copy.start()
    for copy in outs:
        copy.wait()


def solution(mesh):
    n = mesh.shape["dp"]
    chips = n // CORES

    def step(*arrays):
        terms, weights, m, v = (arrays[i : i + NAMES] for i in range(0, 4 * NAMES, NAMES))
        blocks = [one.shape[1:] for one in m]
        sems = lambda *shape: pltpu.SemaphoreType.DMA(shape)
        one_each, full = sems(LAYERS, 2), sems(LAYERS, 2, chips)
        credits = pltpu.SemaphoreType.REGULAR((LAYERS, 2))
        any_space, vmem = (pl.BlockSpec(memory_space=space) for space in (pl.ANY, pltpu.VMEM))
        results = (*weights, *m, *v)
        late = [jax.ShapeDtypeStruct((LAYERS, *blocks[LATE[0]]), jnp.bfloat16)] * LAYERS
        late.append(jax.ShapeDtypeStruct((LAYERS, *blocks[END]), jnp.bfloat16))
        out = pl.pallas_call(
            functools.partial(kernel, n),
            out_shape=[pltpu.VMEM(one.shape, one.dtype) for one in results] + late,
            in_specs=[any_space] * (4 * NAMES),
            out_specs=[vmem] * (3 * NAMES) + [any_space] * len(late),
            scratch_shapes=[
                *(pltpu.VMEM((LAYERS, *b), jnp.bfloat16) for b in blocks),
                full, full, full, full,
                sems(LAYERS, FIRST), one_each, one_each, one_each, one_each, sems(LAYERS),
                full, full, full, full,
                credits, credits,
            ],
            compiler_params=pltpu.CompilerParams(collective_id=0, has_side_effects=True, vmem_limit_bytes=VMEM_LIMIT),
            name="step",
        )(*terms, *weights, *m, *v)

        def hop(i, one):
            by = CORES if i == 0 else n - CORES
            return lax.ppermute(one, "dp", [(a, (a + by) % n) for a in range(n)])

        def across(one):
            return lax.ppermute(one, "dp", [(a, a + 1 - 2 * (a % CORES)) for a in range(n)])

        *tails, end = out[3 * NAMES :]
        come = [hop(i, one) for i, one in enumerate(tails)]
        ends = [end, across(end)]
        shared = [across(one) for one in come]
        done = pl.pallas_call(
            functools.partial(finish, n),
            out_shape=[jax.ShapeDtypeStruct(one.shape, one.dtype) for one in results],
            in_specs=[vmem] * (3 * NAMES),
            out_specs=[any_space] * (3 * NAMES),
            scratch_shapes=[sems(LAYERS * NAMES * (chips + 1))],
            compiler_params=pltpu.CompilerParams(vmem_limit_bytes=VMEM_LIMIT),
            cost_estimate=pl.CostEstimate(flops=20_000_000_000, bytes_accessed=64_000_000, transcendentals=0),
            name="finish",
        )(*(pltpu.with_memory_space_constraint(one, pltpu.VMEM) for one in out[: 3 * NAMES]))
        done = list(done)

        def place(js, sources, space, items):
            blocks_late = [pltpu.with_memory_space_constraint(one, space) for one in sources]
            bounce = [pltpu.VMEM((len(items), *sources[0].shape[1:]), jnp.bfloat16)] if space is pltpu.HBM else []
            placed = pl.pallas_call(
                functools.partial(place_late, n, items, len(sources), len(js)),
                out_shape=[jax.ShapeDtypeStruct(done[j].shape, done[j].dtype) for j in js],
                in_specs=[any_space if bounce else vmem] * len(sources) + [any_space] * len(js),
                out_specs=[any_space] * len(js),
                scratch_shapes=[*bounce, sems(2, len(items))],
                input_output_aliases={len(sources) + i: i for i in range(len(js))},
                compiler_params=pltpu.CompilerParams(vmem_limit_bytes=VMEM_LIMIT),
            )(*blocks_late, *(done[j] for j in js))
            for j, one in zip(js, placed, strict=True):
                done[j] = one

        place((END,), ends, pltpu.HBM, [(i, d, i == 1, 0, d) for i in range(2) for d in range(LAYERS)])
        place(LATE, come, pltpu.HBM, [(i, layer, False, i, i) for layer in range(LAYERS) for i in range(len(LATE))])
        place(LATE, shared, pltpu.VMEM, [(i, layer, True, i, i) for layer in range(LAYERS) for i in range(len(LATE))])
        return tuple(done)

    all_of, cut = P(None, None, None), P(None, "dp", None)
    return jax.shard_map(
        step,
        mesh=mesh,
        in_specs=(P(("rep", "dp"), None, None, None),) * 3 + (all_of,) * 3 + (cut,) * 6,
        out_specs=(P("rep", None, None),) * 3 + (P("rep", "dp", None),) * 6,
        check_vma=False,
    )
```
